256 devices in a mesh: expert: 4 (over y), shard: 64 (over z, x, core).
Axes of the slice: x: 4, y: 4, z: 8, core: 2. Of those that a mesh axis runs over, the one named last changes fastest.
Arguments:
- gradient: bfloat16 [4, 2048, 28672], P('expert', 'shard'), may hold values from -16 to 16
- factor: float32 [4, 2048, 512], P('expert', 'shard'), may hold values from -2 to 2, as said below
- right_diag: float32 [4, 28672], P('expert', 'shard'), may hold values from 0.5 to 2
- counts: int32 [4], P('expert'), may hold values from 256 to 1023
Outputs:
- new_factor: float32 [4, 2048, 512], P('expert', 'shard')
- new_right: float32 [4, 28672], P('expert', 'shard')
The draws below stay inside these ranges and needn't reach their ends.
Inputs may be any that keep to these rules, and one draw needn't show every extreme that they name: Every diagonal block of factor is upper triangular with a positive diagonal: in row r, entry j is zero for j < r % 512.
All inputs are finite; a program needn't handle non-finite values. Where the reference program divides by a largest or mean magnitude, that divisor is 1e-20 or more.
Results may differ from the reference program's by a relative error of at most 0.002.
Values may be sent and summed in bfloat16 or wider, within the bound.
No kernel may reach another device: no remote copies, remote signals or barrier semaphores. Data moves between devices by JAX's collectives and lax.ppermute only.
A program may use at most 128 MiB of HBM per device.

```python
import math
import jax
import jax.numpy as jnp
from jax import lax

D = 2048
FF = 14336
BLOCK = 512
EXPERTS = 4


def draw_factor(key, part):
    base = jax.random.fold_in(key, 11)
    first_key, second_key = jax.random.split(base)
    diagonal = jnp.exp(jax.random.uniform(first_key, (EXPERTS, D, 1), jnp.float32, jnp.log(0.5), jnp.log(2.0)))
    spread = jnp.clip(jax.random.normal(second_key, (EXPERTS, D, BLOCK), jnp.float32), -4.0, 4.0)
    row_place = lax.broadcasted_iota(jnp.int32, (EXPERTS, D, BLOCK), 1) % BLOCK
    column_place = lax.broadcasted_iota(jnp.int32, (EXPERTS, D, BLOCK), 2)
    offdiag = jnp.where(column_place > row_place, spread * (0.6 / jnp.sqrt(jnp.float32(BLOCK))), 0.0)
    return offdiag + jnp.where(column_place == row_place, diagonal, 0.0)


def touch_ends(result, rng, low, high):
    longest = result.shape.index(max(result.shape))
    spots = []
    for shift in (0, 1):
        where = [jax.random.randint(jax.random.fold_in(rng, axis), (), 0, length) for axis, length in enumerate(result.shape)]
        where[longest] = (where[longest] + shift) % result.shape[longest]
        spots.append(tuple(where))
    return result.at[spots[0]].set(low).at[spots[1]].set(high)


def strengthened(drawn, key, source, target, blocks, factor):
    owner, partner = [(jnp.arange(drawn.shape[axis_at]) // (drawn.shape[axis_at] // blocks)).reshape([-1 if axis == axis_at else 1 for axis in range(drawn.ndim)]) for axis_at in (source, target)]
    chosen = jax.random.permutation(key, blocks)[partner]
    strong = (owner == chosen) | (owner == (partner + blocks // 2) % blocks)
    return jnp.where(strong, factor * drawn, drawn)


def block_scale(own_key, shape, shards, least, largest):
    gain = 1.0
    for dim, parts in shards:
        steps = jax.random.uniform(jax.random.fold_in(jax.random.fold_in(own_key, 6), dim), (parts,), jnp.float32, least / len(shards), largest / len(shards))
        gain = gain * jnp.repeat(jnp.exp(steps), shape[dim] // parts).reshape((-1,) + (1,) * (len(shape) - 1 - dim))
    return gain


def bell_draw_with(stream_key, shape, width, reach, cuts, heavy, kind=jnp.bfloat16):
    values = width * jax.random.normal(stream_key, shape, jnp.float32)
    if cuts:
        values = values * block_scale(stream_key, shape, cuts, -0.22, 0.18)
    return jnp.clip(strengthened(values, jax.random.fold_in(stream_key, 3), *heavy), -reach, reach).astype(kind)


def setup_inputs(seed: int = 0) -> dict:
    seeds = jax.random.split(jax.random.key(seed), 5)
    gradient = bell_draw_with(seeds[0], (EXPERTS, D, 2 * FF), 1.0, 16.0, ((0, 4), (1, 64)), (2, 1, 64, 4.0))
    factor = draw_factor(jax.random.fold_in(seeds[4], 71), 0)
    right_diag = jnp.clip(jnp.exp(math.log(2.0) - 1.3862944 * jax.random.uniform(seeds[2], (EXPERTS, 2 * FF), jnp.float32) ** block_scale(seeds[2], (EXPERTS, 2 * FF), ((0, 4), (1, 64)), -0.2, 0.2)), 0.5, 2.0)
    counts = touch_ends(jax.random.randint(seeds[3], (EXPERTS,), 256, 1024), jax.random.fold_in(seeds[3], 1), 256, 1023).astype(jnp.int32)
    return dict(gradient=gradient, factor=factor, right_diag=right_diag, counts=counts)


step_rate = 0.5
epsilon = 1e-6


def reference(gradient, factor, right_diag, counts):
    weight = EXPERTS * counts.astype(jnp.float32) / jnp.sum(counts).astype(jnp.float32)
    blocks = D // BLOCK
    factors_out = []
    rights_out = []
    for expert in range(EXPERTS):
        squared = weight[expert] * weight[expert]
        images = []
        narrows = []
        column_sum = jnp.zeros((2 * FF,), jnp.float32)
        for block_number in range(blocks):
            begin = block_number * BLOCK
            narrow = factor[expert, begin:begin + BLOCK, :].astype(jnp.bfloat16)
            raw = jnp.dot(narrow, gradient[expert, begin:begin + BLOCK, :], preferred_element_type=jnp.float32)
            image = (raw * right_diag[expert][None, :]).astype(jnp.bfloat16)
            column_sum = column_sum + jnp.sum(jnp.square(image.astype(jnp.float32)), axis=0)
            images.append(image)
            narrows.append(narrow)
        column_term = squared * column_sum / D - 1.0
        uppers = []
        row_peak = jnp.float32(0.0)
        for block_number in range(blocks):
            image = images[block_number]
            gram = jnp.dot(image, image.T, preferred_element_type=jnp.float32) * (squared / (2 * FF))
            upper_part = jnp.triu(gram - jnp.eye(BLOCK, dtype=jnp.float32))
            row_peak = jnp.maximum(row_peak, jnp.max(jnp.abs(upper_part)))
            uppers.append(upper_part)
        column_peak = jnp.max(jnp.abs(column_term))
        pieces = []
        for block_number in range(blocks):
            steps = (uppers[block_number] / (row_peak + epsilon)).astype(jnp.bfloat16)
            moved = jnp.dot(steps, narrows[block_number], preferred_element_type=jnp.float32)
            begin = block_number * BLOCK
            pieces.append(factor[expert, begin:begin + BLOCK, :] - step_rate * moved)
        factors_out.append(jnp.concatenate(pieces, axis=0))
        rights_out.append(right_diag[expert] - step_rate * column_term / (column_peak + epsilon) * right_diag[expert])
    return jnp.stack(factors_out), jnp.stack(rights_out)
```

```python
import jax
import jax.numpy as jnp
from jax import lax
from jax.experimental import pallas as pl
from jax.experimental.pallas import tpu as pltpu
from jax.sharding import Mesh
from jax.sharding import PartitionSpec as P

SHARD = ("zh", "zl", "x", "c")
GROUP = ("zl", "x", "c")
CROSS = ("zh", "c")
FF2 = 28672
DIM = 2048
BLOCK = 512
ROWS = 32
OWN = 448
PAIR = 896
WIDE = 1792
MESSAGE = BLOCK + WIDE

step_rate = 0.5
epsilon = 1e-06

VMEM = pl.BlockSpec(memory_space=pltpu.VMEM)
SMEM = pl.BlockSpec(memory_space=pltpu.SMEM)


def pack_kernel(gradient, factor, out):
    narrow = factor[0].astype(jnp.bfloat16)
    for place in range(8):
        for core in range(2):
            dest = place * 2 + core
            out[dest, :, :BLOCK] = narrow
            for q in range(2):
                begin = ((2 * core + q) * 16 + place * 2) * OWN
                left = BLOCK + q * PAIR
                out[dest, :, left : left + PAIR] = gradient[0, :, begin : begin + PAIR]


def gram_kernel(places, scales, got, rights, part, sums, image):
    core = places[0]
    mine = jnp.where(core == 0, rights[0:4, :], rights[4:8, :])
    right = jnp.concatenate([mine[k : k + 1, :] for k in range(4)], axis=1)
    upper_left = got[0:256, 0:512]
    lower_right = got[256:512, 256:512]
    totals = []
    for k in range(7):
        at = BLOCK + k * 256
        scale = right[:, k * 256 : (k + 1) * 256]
        high = jnp.dot(upper_left, got[:, at : at + 256], preferred_element_type=jnp.float32)
        low = jnp.dot(lower_right, got[256:512, at : at + 256], preferred_element_type=jnp.float32)
        high = (high * scale).astype(jnp.bfloat16)
        low = (low * scale).astype(jnp.bfloat16)
        image[0:256, k * 256 : (k + 1) * 256] = high
        image[256:512, k * 256 : (k + 1) * 256] = low
        total = jnp.sum(jnp.square(high.astype(jnp.float32)), axis=0, keepdims=True)
        total = total + jnp.sum(jnp.square(low.astype(jnp.float32)), axis=0, keepdims=True)
        totals.append(total)
    total = jnp.concatenate(totals, axis=1)
    row = lax.broadcasted_iota(jnp.int32, (8, PAIR), 0)
    chosen = jnp.where((row // 2) % 2 == 0, total[:, :PAIR], total[:, PAIR:])
    sums[...] = jnp.where(row // 4 == core, chosen, 0.0)
    last = (((1,), (1,)), ((), ()))
    scale = scales[1]
    high = lax.dot_general(image[0:256, :], image[...], last, preferred_element_type=jnp.float32)
    low = lax.dot_general(image[256:512, :], image[256:512, :], last, preferred_element_type=jnp.float32)
    share = jnp.float32(1.0 / 16.0)
    row_high = lax.broadcasted_iota(jnp.int32, (256, 512), 0)
    col_high = lax.broadcasted_iota(jnp.int32, (256, 512), 1)
    row_low = lax.broadcasted_iota(jnp.int32, (256, 256), 0)
    col_low = lax.broadcasted_iota(jnp.int32, (256, 256), 1)
    part[0:256, :] = (high * scale - jnp.where(row_high == col_high, share, 0.0)).astype(part.dtype)
    part[256:512, 256:512] = (low * scale - jnp.where(row_low == col_low, share, 0.0)).astype(part.dtype)
    part[256:512, 0:256] = jnp.zeros((256, 256), part.dtype)


def peaks_kernel(places, scales, parts, sums, upper, term, levels):
    core, first = places[0], places[1]
    total = parts[0].astype(jnp.float32)
    for k in range(1, 16):
        total = total + parts[k].astype(jnp.float32)
    row = lax.broadcasted_iota(jnp.int32, (ROWS, BLOCK), 0) + first
    col = lax.broadcasted_iota(jnp.int32, (ROWS, BLOCK), 1)
    total = jnp.where(col >= row, total, 0.0)
    upper[...] = total
    row_level = jnp.max(jnp.abs(total))
    added = jnp.sum(sums[...], axis=0, keepdims=True)
    added = jnp.where(core == 0, added[:, :OWN], added[:, OWN:])
    column_term = scales[0] * added / DIM - 1.0
    term[...] = column_term
    column_level = jnp.max(jnp.abs(column_term))
    lane = lax.broadcasted_iota(jnp.int32, levels.shape, 2)
    levels[...] = jnp.where(lane == 0, row_level, column_level)


def final_kernel(levels, upper, narrow, factor, term, right, new_factor, new_right):
    peak = jnp.max(levels[...], axis=0)
    row_peak = jnp.max(peak[0:1, 0:1])
    column_peak = jnp.max(peak[0:1, 1:2])
    steps = (upper[...] / (row_peak + epsilon)).astype(jnp.bfloat16)
    moved = jnp.dot(steps, narrow[...], preferred_element_type=jnp.float32)
    new_factor[0] = factor[0] - step_rate * moved
    new_right[...] = right[...] - step_rate * term[...] / (column_peak + epsilon) * right[...]


def shape(dims, dtype=jnp.float32):
    return jax.ShapeDtypeStruct(dims, dtype)


def cost(flops, moved):
    return pl.CostEstimate(flops=flops, bytes_accessed=moved, transcendentals=0)


def body(gradient, factor, right_diag, counts):
    packed = pl.pallas_call(
        pack_kernel,
        out_shape=shape((16, ROWS, MESSAGE), jnp.bfloat16),
        in_specs=[VMEM, VMEM],
        out_specs=VMEM,
        cost_estimate=cost(1000000, 4194304),
        name="pack",
    )(gradient, factor)
    got = lax.all_to_all(packed, GROUP, 0, 0, tiled=True).reshape(BLOCK, MESSAGE)
    rights = lax.all_to_all(jnp.broadcast_to(right_diag, (8, OWN)), CROSS, 0, 0, tiled=True)
    tokens = lax.all_to_all(jnp.broadcast_to(counts, (4,)), "expert", 0, 0, tiled=True)
    weight = 4 * counts.astype(jnp.float32) / jnp.sum(tokens).astype(jnp.float32)
    squared = weight * weight
    scales = jnp.concatenate([squared, squared / FF2])
    core = lax.axis_index("c")
    first = lax.axis_index(GROUP) * ROWS
    places = jnp.stack([core, first]).astype(jnp.int32)
    part, sums = pl.pallas_call(
        gram_kernel,
        out_shape=[shape((BLOCK, BLOCK), jnp.bfloat16), shape((8, PAIR))],
        in_specs=[SMEM, SMEM, VMEM, VMEM],
        out_specs=[VMEM, VMEM],
        scratch_shapes=[pltpu.VMEM((BLOCK, WIDE), jnp.bfloat16)],
        cost_estimate=cost(1600000000, 4194304),
        name="gram",
    )(places, scales, got, rights)
    parts = lax.all_to_all(part.reshape(16, ROWS, BLOCK), GROUP, 0, 0, tiled=True)
    sums = lax.all_to_all(sums, CROSS, 0, 0, tiled=True)
    upper, term, levels = pl.pallas_call(
        peaks_kernel,
        out_shape=[shape((ROWS, BLOCK)), shape((1, OWN)), shape((64, 1, 128))],
        in_specs=[SMEM, SMEM, VMEM, VMEM],
        out_specs=[VMEM, VMEM, VMEM],
        cost_estimate=cost(1000000, 1048576),
        name="peaks",
    )(places, scales, parts, sums)
    levels = lax.all_to_all(levels, SHARD, 0, 0, tiled=True)
    new_factor, new_right = pl.pallas_call(
        final_kernel,
        out_shape=[shape((1, ROWS, BLOCK)), shape((1, OWN))],
        grid=(1,),
        in_specs=[
            VMEM,
            VMEM,
            pl.BlockSpec((BLOCK, BLOCK), lambda i: (0, 0)),
            VMEM,
            VMEM,
            VMEM,
        ],
        out_specs=[VMEM, VMEM],
        cost_estimate=cost(17000000, 1048576),
        name="final",
    )(levels, upper, got, factor, term, right_diag)
    return new_factor, new_right


def solution(mesh):
    torus = Mesh(
        mesh.devices.reshape(mesh.shape["expert"], 4, 2, 4, 2),
        ("expert", "zh", "zl", "x", "c"),
    )
    return jax.shard_map(
        body,
        mesh=torus,
        in_specs=(
            P("expert", SHARD, None),
            P("expert", SHARD, None),
            P("expert", SHARD),
            P("expert"),
        ),
        out_specs=(P("expert", SHARD, None), P("expert", SHARD)),
        check_vma=False,
    )
```

```python
import jax
import jax.numpy as jnp
from jax import lax
from jax.experimental import pallas as pl
from jax.experimental.pallas import tpu as pltpu
from jax.sharding import Mesh
from jax.sharding import PartitionSpec as P


SHARD = ("zh", "zl", "x", "c")
GROUP = ("zl", "x", "c")
FF2 = 28672
DIM = 2048
BLOCK = 512
ROWS = 32
OWN = 448
PAIR = 896
SPAN = 16 * OWN
WIDE = 1792
MESSAGE = BLOCK + WIDE

step_rate = 0.5
epsilon = 1e-06


VMEM = pl.BlockSpec(memory_space=pltpu.VMEM)
HBM = pl.BlockSpec(memory_space=pltpu.HBM)
SMEM = pl.BlockSpec(memory_space=pltpu.SMEM)


def pack_kernel(gradient, factor, out, near, rows, message, in_sems, out_sems):
    block = lax.axis_index("zh")
    fetches = [pltpu.make_async_copy(factor, rows, in_sems.at[4])]
    for d in range(4):
        begin = pl.multiple_of(lax.rem(block + (4 - d), 4) * SPAN, 128)
        source = gradient.at[0, :, pl.ds(begin, SPAN)]
        fetches.append(pltpu.make_async_copy(source, near.at[d], in_sems.at[d]))
    for fetch in fetches:
        fetch.start()
    fetches[0].wait()
    narrow = rows[0].astype(jnp.bfloat16)
    for dest in range(16):
        message[dest, :, :BLOCK] = narrow
    sends = []
    for q in range(2):
        fetches[1 + 2 * q].wait()
        fetches[2 + 2 * q].wait()
        left = BLOCK + q * PAIR
        for part in range(2):
            for place in range(4 * part, 4 * part + 4):
                pairs = [near[2 * q + k, :, place * PAIR : (place + 1) * PAIR] for k in range(2)]
                for core in range(2):
                    pieces = [pair[:, core * OWN : (core + 1) * OWN] for pair in pairs]
                    message[place * 2 + core, :, left : left + PAIR] = jnp.concatenate(pieces, axis=1)
            begin = 0 if q == 0 else left
            view = (pl.ds(8 * part, 8), slice(None), pl.ds(begin, left + PAIR - begin))
            send = pltpu.make_async_copy(message.at[view], out.at[view], out_sems.at[2 * q + part])
            send.start()
            sends.append(send)
    for send in sends:
        send.wait()


def gram_kernel(scales, got, right0, right1, right2, right3, part, sum0, sum1, sum2, sum3, image):
    right = jnp.concatenate([right0[...], right1[...], right2[...], right3[...]], axis=1)
    upper_left = got[0:256, 0:512]
    lower_right = got[256:512, 256:512]
    totals = []
    for k in range(7):
        at = BLOCK + k * 256
        scale = right[:, k * 256 : (k + 1) * 256]
        high = jnp.dot(upper_left, got[:, at : at + 256], preferred_element_type=jnp.float32)
        low = jnp.dot(lower_right, got[256:512, at : at + 256], preferred_element_type=jnp.float32)
        high = (high * scale).astype(jnp.bfloat16)
        low = (low * scale).astype(jnp.bfloat16)
        image[0:256, k * 256 : (k + 1) * 256] = high
        image[256:512, k * 256 : (k + 1) * 256] = low
        total = jnp.sum(jnp.square(high.astype(jnp.float32)), axis=0, keepdims=True)
        total = total + jnp.sum(jnp.square(low.astype(jnp.float32)), axis=0, keepdims=True)
        totals.append(total)
    total = jnp.concatenate(totals, axis=1)
    for d, out in enumerate((sum0, sum1, sum2, sum3)):
        out[...] = total[:, d * OWN : (d + 1) * OWN]
    last = (((1,), (1,)), ((), ()))
    scale = scales[1]
    high = lax.dot_general(image[0:256, :], image[...], last, preferred_element_type=jnp.float32)
    low = lax.dot_general(image[256:512, :], image[256:512, :], last, preferred_element_type=jnp.float32)
    share = jnp.float32(1.0 / 16.0)
    row_high = lax.broadcasted_iota(jnp.int32, (256, 512), 0)
    col_high = lax.broadcasted_iota(jnp.int32, (256, 512), 1)
    row_low = lax.broadcasted_iota(jnp.int32, (256, 256), 0)
    col_low = lax.broadcasted_iota(jnp.int32, (256, 256), 1)
    part[0:256, :] = (high * scale - jnp.where(row_high == col_high, share, 0.0)).astype(part.dtype)
    part[256:512, 256:512] = (low * scale - jnp.where(row_low == col_low, share, 0.0)).astype(part.dtype)
    part[256:512, 0:256] = jnp.zeros((256, 256), part.dtype)


def peaks_kernel(scales, parts, sum0, sum1, sum2, sum3, upper, term, levels):
    first = lax.axis_index(GROUP) * ROWS
    total = parts[0].astype(jnp.float32)
    for k in range(1, 16):
        total = total + parts[k].astype(jnp.float32)
    row = lax.broadcasted_iota(jnp.int32, (ROWS, BLOCK), 0) + first
    col = lax.broadcasted_iota(jnp.int32, (ROWS, BLOCK), 1)
    total = jnp.where(col >= row, total, 0.0)
    upper[...] = total
    row_level = jnp.max(jnp.abs(total))
    added = (sum0[...] + sum1[...]) + (sum2[...] + sum3[...])
    column_term = scales[0] * added / DIM - 1.0
    term[...] = column_term
    column_level = jnp.max(jnp.abs(column_term))
    lane = lax.broadcasted_iota(jnp.int32, levels.shape, 2)
    levels[...] = jnp.where(lane == 0, row_level, column_level)


def final_kernel(levels, upper, narrow, factor, term, right, new_factor, new_right):
    peak = jnp.max(levels[...], axis=0)
    row_peak = jnp.max(peak[0:1, 0:1])
    column_peak = jnp.max(peak[0:1, 1:2])
    steps = (upper[...] / (row_peak + epsilon)).astype(jnp.bfloat16)
    moved = jnp.dot(steps, narrow[...], preferred_element_type=jnp.float32)
    new_factor[0] = factor[0] - step_rate * moved
    new_right[...] = right[...] - step_rate * term[...] / (column_peak + epsilon) * right[...]


def shape(dims, dtype=jnp.float32):
    return jax.ShapeDtypeStruct(dims, dtype)


def call(kernel, ins, outs, flops, scratch=(), room=16):
    return pl.pallas_call(
        kernel,
        out_shape=outs,
        grid=(1,),
        in_specs=ins,
        out_specs=[VMEM] * len(outs),
        scratch_shapes=list(scratch),
        compiler_params=pltpu.CompilerParams(vmem_limit_bytes=room * 1024 * 1024),
        cost_estimate=pl.CostEstimate(flops=flops, bytes_accessed=2097152, transcendentals=0),
    )


def exchange(value, axes):
    return lax.all_to_all(value, axes, 0, 0, tiled=True)


def shifted(value, axis, by):
    size = lax.axis_size(axis)
    return lax.ppermute(value, axis, [(k, (k + by) % size) for k in range(size)])


def inner(gradient, factor, right_diag, counts):
    half = jnp.bfloat16
    packed = pl.pallas_call(
        pack_kernel,
        out_shape=shape((16, ROWS, MESSAGE), half),
        in_specs=[HBM, HBM],
        out_specs=HBM,
        scratch_shapes=[
            pltpu.VMEM((4, ROWS, SPAN), half),
            pltpu.VMEM((1, ROWS, BLOCK), jnp.float32),
            pltpu.VMEM((16, ROWS, MESSAGE), half),
            pltpu.SemaphoreType.DMA((5,)),
            pltpu.SemaphoreType.DMA((4,)),
        ],
        compiler_params=pltpu.CompilerParams(vmem_limit_bytes=62 * 1024 * 1024),
        cost_estimate=pl.CostEstimate(flops=2000000, bytes_accessed=4194304, transcendentals=0),
        name="pack",
    )(gradient, factor)
    got = exchange(packed, GROUP).reshape(BLOCK, MESSAGE)
    rights = [right_diag] + [shifted(right_diag, "zh", d) for d in (1, 2, 3)]
    tokens = counts
    for d in (1, 2, 3):
        tokens = tokens + shifted(counts, "expert", d)
    weight = 4 * counts.astype(jnp.float32) / tokens.astype(jnp.float32)
    squared = weight * weight
    scales = jnp.concatenate([squared, squared / FF2])
    part, *sums = call(
        gram_kernel,
        [SMEM] + [VMEM] * 5,
        [shape((BLOCK, BLOCK), half)] + [shape((1, OWN))] * 4,
        1600000000,
        [pltpu.VMEM((BLOCK, WIDE), half)],
    )(scales, got, *rights)
    parts = exchange(part.reshape(16, ROWS, BLOCK), GROUP)
    sums = [sums[0]] + [shifted(sums[d], "zh", -d) for d in (1, 2, 3)]
    upper, term, levels = call(
        peaks_kernel,
        [SMEM] + [VMEM] * 5,
        [shape((ROWS, BLOCK)), shape((1, OWN)), shape((64, 1, 128))],
        2000000,
    )(scales, parts, *sums)
    levels = exchange(levels, SHARD)
    new_factor, new_right = call(
        final_kernel,
        [VMEM, VMEM, pl.BlockSpec((BLOCK, BLOCK), lambda i: (0, 0)), VMEM, VMEM, VMEM],
        [shape((1, ROWS, BLOCK)), shape((1, OWN))],
        17000000,
    )(levels, upper, got, factor, term, right_diag)
    return new_factor, new_right


def solution(mesh):
    torus = Mesh(
        mesh.devices.reshape(mesh.shape["expert"], 4, 2, 4, 2),
        ("expert", "zh", "zl", "x", "c"),
    )
    return jax.shard_map(
        inner,
        mesh=torus,
        in_specs=(
            P("expert", SHARD, None),
            P("expert", SHARD, None),
            P("expert", SHARD),
            P("expert"),
        ),
        out_specs=(P("expert", SHARD, None), P("expert", SHARD)),
        check_vma=False,
    )
```

```python
import jax
import jax.numpy as jnp
from jax import lax
from jax.experimental import pallas as pl
from jax.experimental.pallas import tpu as pltpu
from jax.sharding import Mesh
from jax.sharding import PartitionSpec as P


SHARD = ("zh", "zl", "x", "c")
GROUP = ("zl", "x", "c")
FF2 = 28672
DIM = 2048
BLOCK = 512
ROWS = 32
OWN = 448
PAIR = 896
SPAN = 16 * OWN
HALF = 8 * OWN
OFFSETS = (
    (1, 0, 0), (0, 2, 0), (1, 0, 1), (0, 2, 1), (1, 1, 0), (0, 3, 0), (1, 3, 0), (0, 1, 0),
    (1, 1, 1), (0, 3, 1), (1, 3, 1), (0, 1, 1), (1, 2, 0), (1, 2, 1), (0, 0, 1), (0, 0, 0),
)
PEERS = len(OFFSETS)
WIDE = 1792
MESSAGE = BLOCK + WIDE

step_rate = 0.5
epsilon = 1e-06


VMEM = pl.BlockSpec(memory_space=pltpu.VMEM)
HBM = pl.BlockSpec(memory_space=pltpu.HBM)
SMEM = pl.BlockSpec(memory_space=pltpu.SMEM)


def pack_kernel(gradient, factor, counts, *refs):
    outs, notes, (near, rows, sems) = refs[:PEERS], refs[PEERS], refs[PEERS + 1 :]
    block, plane = lax.axis_index("zh"), lax.axis_index("zl")
    x, c = lax.axis_index("x"), lax.axis_index("c")
    fetches = [pltpu.make_async_copy(factor, rows, sems.at[8])]
    for dz in range(2):
        for d in range(4):
            begin = pl.multiple_of((block ^ d) * SPAN + lax.rem(plane + dz, 2) * HALF, 128)
            source = gradient.at[0, :, pl.ds(begin, HALF)]
            fetches.append(pltpu.make_async_copy(source, near.at[dz, d], sems.at[4 * dz + d]))
    for fetch in fetches:
        fetch.start()
    notes[...] = jnp.full(notes.shape, counts[0].astype(jnp.float32), jnp.float32)
    fetches[0].wait()
    narrow = rows[0].astype(jnp.bfloat16)
    for out in outs:
        out[:, :BLOCK] = narrow
    for dz in range(2):
        for fetch in fetches[1 + 4 * dz : 5 + 4 * dz]:
            fetch.wait()
        for dx in range(4):
            begin = pl.multiple_of(lax.rem(x + dx, 4) * PAIR, 128)
            same, other = outs[OFFSETS.index((dz, dx, 0))], outs[OFFSETS.index((dz, dx, 1))]
            for q in range(2):
                pairs = [near[dz, 2 * q + k, :, pl.ds(begin, PAIR)] for k in range(2)]
                even = jnp.concatenate([pair[:, :OWN] for pair in pairs], axis=1)
                odd = jnp.concatenate([pair[:, OWN:] for pair in pairs], axis=1)
                left = BLOCK + q * PAIR
                same[:, left : left + PAIR] = jnp.where(c == 0, even, odd)
                other[:, left : left + PAIR] = jnp.where(c == 0, odd, even)


def gram_kernel(*refs):
    rights, tokens, staying = refs[0:4], refs[4:8], refs[8]
    crosses, refs = refs[9 : PEERS + 8], refs[9:]
    part, sum0, sum1, sum2, sum3, narrow, level, got, image = refs[PEERS - 1 :]
    plane, x, c = lax.axis_index("zl"), lax.axis_index("x"), lax.axis_index("c")
    own = pl.multiple_of((plane * 8 + x * 2 + c) * ROWS, ROWS)
    got[pl.ds(own, ROWS), :] = staying[...]
    total = (tokens[0][...] + tokens[1][...]) + (tokens[2][...] + tokens[3][...])
    weight = (4 * tokens[0][...] / total)[:, 0:1]
    squared = weight * weight
    level[...] = jnp.broadcast_to(squared, level.shape)
    for k, (dz, dx, dc) in enumerate(OFFSETS[:-1]):
        source = lax.rem(plane + dz, 2) * 8 + lax.rem(x + (4 - dx), 4) * 2 + lax.rem(c + dc, 2)
        got[pl.ds(pl.multiple_of(source * ROWS, ROWS), ROWS), :] = crosses[k][...]
    narrow[...] = got[:, :BLOCK]
    right = jnp.concatenate([one[...] for one in rights], axis=1)
    upper_left = got[0:256, 0:512]
    lower_right = got[256:512, 256:512]
    totals = []
    for k in range(7):
        at = BLOCK + k * 256
        scale = right[:, k * 256 : (k + 1) * 256]
        high = jnp.dot(upper_left, got[:, at : at + 256], preferred_element_type=jnp.float32)
        low = jnp.dot(lower_right, got[256:512, at : at + 256], preferred_element_type=jnp.float32)
        high = (high * scale).astype(jnp.bfloat16)
        low = (low * scale).astype(jnp.bfloat16)
        image[0:256, k * 256 : (k + 1) * 256] = high
        image[256:512, k * 256 : (k + 1) * 256] = low
        total = jnp.sum(jnp.square(high.astype(jnp.float32)), axis=0, keepdims=True)
        total = total + jnp.sum(jnp.square(low.astype(jnp.float32)), axis=0, keepdims=True)
        totals.append(total)
    total = jnp.concatenate(totals, axis=1)
    for d, out in enumerate((sum0, sum1, sum2, sum3)):
        out[...] = total[:, d * OWN : (d + 1) * OWN]
    last = (((1,), (1,)), ((), ()))
    scale = squared / FF2
    high = lax.dot_general(image[0:256, :], image[...], last, preferred_element_type=jnp.float32)
    low = lax.dot_general(image[256:512, :], image[256:512, :], last, preferred_element_type=jnp.float32)
    share = jnp.float32(1.0 / 16.0)
    row_high = lax.broadcasted_iota(jnp.int32, (256, 512), 0)
    col_high = lax.broadcasted_iota(jnp.int32, (256, 512), 1)
    row_low = lax.broadcasted_iota(jnp.int32, (256, 256), 0)
    col_low = lax.broadcasted_iota(jnp.int32, (256, 256), 1)
    part[0:256, :] = (high * scale - jnp.where(row_high == col_high, share, 0.0)).astype(part.dtype)
    part[256:512, 256:512] = (low * scale - jnp.where(row_low == col_low, share, 0.0)).astype(part.dtype)
    part[256:512, 0:256] = jnp.zeros((256, 256), part.dtype)


def peaks_kernel(squared, parts, sum0, sum1, sum2, sum3, upper, term, levels):
    first = lax.axis_index(GROUP) * ROWS
    total = parts[0].astype(jnp.float32)
    for k in range(1, 16):
        total = total + parts[k].astype(jnp.float32)
    row = lax.broadcasted_iota(jnp.int32, (ROWS, BLOCK), 0) + first
    col = lax.broadcasted_iota(jnp.int32, (ROWS, BLOCK), 1)
    total = jnp.where(col >= row, total, 0.0)
    upper[...] = total
    row_level = jnp.max(jnp.abs(total))
    added = (sum0[...] + sum1[...]) + (sum2[...] + sum3[...])
    column_term = squared[0:1, 0:1] * added / DIM - 1.0
    term[...] = column_term
    column_level = jnp.max(jnp.abs(column_term))
    lane = lax.broadcasted_iota(jnp.int32, levels.shape, 2)
    levels[...] = jnp.where(lane == 0, row_level, column_level)


def final_kernel(levels, upper, narrow, factor, term, right, new_factor, new_right):
    peak = jnp.max(levels[...], axis=0)
    row_peak = jnp.max(peak[0:1, 0:1])
    column_peak = jnp.max(peak[0:1, 1:2])
    steps = (upper[...] / (row_peak + epsilon)).astype(jnp.bfloat16)
    moved = jnp.dot(steps, narrow[...], preferred_element_type=jnp.float32)
    new_factor[0] = factor[0] - step_rate * moved
    new_right[...] = right[...] - step_rate * term[...] / (column_peak + epsilon) * right[...]


def shape(dims, dtype=jnp.float32):
    return jax.ShapeDtypeStruct(dims, dtype)


def call(kernel, ins, outs, flops, scratch=(), room=16):
    return pl.pallas_call(
        kernel,
        out_shape=outs,
        grid=(1,),
        in_specs=ins,
        out_specs=[VMEM] * len(outs),
        scratch_shapes=list(scratch),
        compiler_params=pltpu.CompilerParams(vmem_limit_bytes=room * 1024 * 1024),
        cost_estimate=pl.CostEstimate(flops=flops, bytes_accessed=2097152, transcendentals=0),
    )


def exchange(value, axes):
    return lax.all_to_all(value, axes, 0, 0, tiled=True)


def across(value, turn, axis="zh"):
    return lax.ppermute(value, axis, [(k, k ^ turn) for k in range(4)])


def to_peer(value, dz, dx, dc):
    pairs = []
    for device in range(16):
        plane, x, c = device // 8, device // 2 % 4, device % 2
        pairs.append((device, (plane + dz) % 2 * 8 + (x + dx) % 4 * 2 + (c + dc) % 2))
    return lax.ppermute(value, GROUP, pairs)


def pack(gradient, factor, counts):
    half = jnp.bfloat16
    outs = [shape((ROWS, MESSAGE), half)] * PEERS
    return pl.pallas_call(
        pack_kernel,
        out_shape=outs + [shape((1, 128))],
        in_specs=[HBM, HBM, SMEM],
        out_specs=[VMEM] * (PEERS + 1),
        scratch_shapes=[
            pltpu.VMEM((2, 4, ROWS, HALF), half),
            pltpu.VMEM((1, ROWS, BLOCK), jnp.float32),
            pltpu.SemaphoreType.DMA((9,)),
        ],
        compiler_params=pltpu.CompilerParams(vmem_limit_bytes=51 * 1024 * 1024),
        cost_estimate=pl.CostEstimate(flops=2000000, bytes_accessed=4194304, transcendentals=0),
        name="pack",
    )(gradient, factor, counts)


def inner(gradient, factor, right_diag, counts):
    half = jnp.bfloat16
    *leaving, staying, token = pack(gradient, factor, counts)
    crosses = [to_peer(value, *OFFSETS[k]) for k, value in enumerate(leaving)]
    rights = [right_diag] + [across(right_diag, d) for d in (1, 2, 3)]
    tokens = [token] + [across(token, d, "expert") for d in (1, 2, 3)]
    part, *sums, narrow, squared = call(
        gram_kernel,
        [VMEM] * (PEERS + 8),
        [shape((BLOCK, BLOCK), half)] + [shape((1, OWN))] * 4 + [shape((BLOCK, BLOCK), half), shape((1, 128))],
        1600000000,
        [pltpu.VMEM((BLOCK, MESSAGE), half), pltpu.VMEM((BLOCK, WIDE), half)],
    )(*rights, *tokens, staying, *crosses)
    parts = exchange(part.reshape(16, ROWS, BLOCK), GROUP)
    sums = [sums[0]] + [across(sums[d], d) for d in (1, 2, 3)]
    upper, term, levels = call(
        peaks_kernel,
        [VMEM] * 6,
        [shape((ROWS, BLOCK)), shape((1, OWN)), shape((64, 1, 128))],
        2000000,
    )(squared, parts, *sums)
    levels = exchange(levels, SHARD)
    new_factor, new_right = call(
        final_kernel, [VMEM] * 6, [shape((1, ROWS, BLOCK)), shape((1, OWN))], 17000000
    )(levels, upper, narrow, factor, term, right_diag)
    return new_factor, new_right


def solution(mesh):
    torus = Mesh(
        mesh.devices.reshape(mesh.shape["expert"], 4, 2, 4, 2),
        ("expert", "zh", "zl", "x", "c"),
    )
    return jax.shard_map(
        inner,
        mesh=torus,
        in_specs=(
            P("expert", SHARD, None),
            P("expert", SHARD, None),
            P("expert", SHARD),
            P("expert"),
        ),
        out_specs=(P("expert", SHARD, None), P("expert", SHARD)),
        check_vma=False,
    )
```

```python
import jax
import jax.numpy as jnp
from jax import lax
from jax.experimental import pallas as pl
from jax.experimental.pallas import tpu as pltpu
from jax.sharding import Mesh
from jax.sharding import PartitionSpec as P


SHARD = ("zh", "zl", "x", "c")
GROUP = ("zl", "x", "c")
FF2 = 28672
DIM = 2048
BLOCK = 512
ROWS = 32
OWN = 448
PAIR = 896
SPAN = 16 * OWN
HALF = 8 * OWN
OFFSETS = (
    (1, 0, 0), (0, 2, 0), (1, 0, 1), (0, 2, 1), (1, 1, 0), (0, 3, 0), (1, 3, 0), (0, 1, 0),
    (1, 1, 1), (0, 3, 1), (1, 3, 1), (0, 1, 1), (1, 2, 0), (1, 2, 1), (0, 0, 1), (0, 0, 0),
)
PEERS = len(OFFSETS)
WIDE = 1792
MESSAGE = BLOCK + WIDE

step_rate = 0.5
epsilon = 1e-06


VMEM = pl.BlockSpec(memory_space=pltpu.VMEM)
HBM = pl.BlockSpec(memory_space=pltpu.HBM)
SMEM = pl.BlockSpec(memory_space=pltpu.SMEM)


def pack_kernel(gradient, factor, counts, *refs):
    outs, notes, (near, rows, sems) = refs[:PEERS], refs[PEERS], refs[PEERS + 1 :]
    block, plane = lax.axis_index("zh"), lax.axis_index("zl")
    x, c = lax.axis_index("x"), lax.axis_index("c")
    fetches = [pltpu.make_async_copy(factor, rows, sems.at[8])]
    for dz in range(2):
        for d in range(4):
            begin = pl.multiple_of((block ^ d) * SPAN + lax.rem(plane + dz, 2) * HALF, 128)
            source = gradient.at[0, :, pl.ds(begin, HALF)]
            fetches.append(pltpu.make_async_copy(source, near.at[dz, d], sems.at[4 * dz + d]))
    for fetch in fetches:
        fetch.start()
    notes[...] = jnp.full(notes.shape, counts[0].astype(jnp.float32), jnp.float32)
    fetches[0].wait()
    narrow = rows[0].astype(jnp.bfloat16)
    for out in outs:
        out[:, :BLOCK] = narrow
    for dz in range(2):
        for fetch in fetches[1 + 4 * dz : 5 + 4 * dz]:
            fetch.wait()
        for dx in range(4):
            begin = pl.multiple_of(lax.rem(x + dx, 4) * PAIR, 128)
            same, other = outs[OFFSETS.index((dz, dx, 0))], outs[OFFSETS.index((dz, dx, 1))]
            for q in range(2):
                pairs = [near[dz, 2 * q + k, :, pl.ds(begin, PAIR)] for k in range(2)]
                even = jnp.concatenate([pair[:, :OWN] for pair in pairs], axis=1)
                odd = jnp.concatenate([pair[:, OWN:] for pair in pairs], axis=1)
                left = BLOCK + q * PAIR
                same[:, left : left + PAIR] = jnp.where(c == 0, even, odd)
                other[:, left : left + PAIR] = jnp.where(c == 0, odd, even)


def gram_kernel(*refs):
    rights, staying = refs[0:4], refs[4]
    crosses, refs = refs[5 : PEERS + 4], refs[5:]
    part, sum0, sum1, sum2, sum3, narrow, got, image = refs[PEERS - 1 :]
    plane, x, c = lax.axis_index("zl"), lax.axis_index("x"), lax.axis_index("c")
    own = pl.multiple_of((plane * 8 + x * 2 + c) * ROWS, ROWS)
    got[pl.ds(own, ROWS), :] = staying[...]
    for k, (dz, dx, dc) in enumerate(OFFSETS[:-1]):
        source = lax.rem(plane + dz, 2) * 8 + lax.rem(x + (4 - dx), 4) * 2 + lax.rem(c + dc, 2)
        got[pl.ds(pl.multiple_of(source * ROWS, ROWS), ROWS), :] = crosses[k][...]
    narrow[...] = got[:, :BLOCK]
    right = jnp.concatenate([one[...] for one in rights], axis=1)
    upper_left = got[0:256, 0:512]
    lower_right = got[256:512, 256:512]
    totals = []
    for k in range(7):
        at = BLOCK + k * 256
        scale = right[:, k * 256 : (k + 1) * 256]
        high = jnp.dot(upper_left, got[:, at : at + 256], preferred_element_type=jnp.float32)
        low = jnp.dot(lower_right, got[256:512, at : at + 256], preferred_element_type=jnp.float32)
        high = (high * scale).astype(jnp.bfloat16)
        low = (low * scale).astype(jnp.bfloat16)
        image[0:256, k * 256 : (k + 1) * 256] = high
        image[256:512, k * 256 : (k + 1) * 256] = low
        total = jnp.sum(jnp.square(high.astype(jnp.float32)), axis=0, keepdims=True)
        total = total + jnp.sum(jnp.square(low.astype(jnp.float32)), axis=0, keepdims=True)
        totals.append(total)
    total = jnp.concatenate(totals, axis=1)
    for d, out in enumerate((sum0, sum1, sum2, sum3)):
        out[...] = total[:, d * OWN : (d + 1) * OWN]
    last = (((1,), (1,)), ((), ()))
    high = lax.dot_general(image[0:256, :], image[...], last, preferred_element_type=jnp.float32)
    low = lax.dot_general(image[256:512, :], image[256:512, :], last, preferred_element_type=jnp.float32)
    places = [[lax.broadcasted_iota(jnp.int32, half.shape, k) for k in range(2)] for half in (high, low)]
    least = [jnp.min(jnp.where(row == col, half, jnp.inf)) for half, (row, col) in zip((high, low), places)]
    share = jnp.full((8, 128), jnp.minimum(*least), jnp.float32).astype(part.dtype).astype(jnp.float32)[0:1, 0:1]
    shared = []
    for half, (row, col) in zip((high, low), places):
        half = jnp.where(row == col, half - share, half)
        slot = jnp.logical_and(row % ROWS == ROWS - 1, col == row - (ROWS - 1))
        shared.append(jnp.where(slot, share, half).astype(part.dtype))
    part[0:256, :], part[256:512, 256:512] = shared
    part[256:512, 0:256] = jnp.zeros((256, 256), part.dtype)


def peaks_kernel(parts, sum0, sum1, sum2, sum3, upper, sums, levels):
    first = lax.axis_index(GROUP) * ROWS
    total = parts[0].astype(jnp.float32)
    for k in range(1, 16):
        total = total + parts[k].astype(jnp.float32)
    place = lax.broadcasted_iota(jnp.int32, (ROWS, BLOCK), 0)
    row = place + first
    col = lax.broadcasted_iota(jnp.int32, (ROWS, BLOCK), 1)
    share = jnp.sum(jnp.where(jnp.logical_and(place == ROWS - 1, col == first), total, 0.0))
    diagonal = total + share
    above, on = col > row, col == row
    upper[...] = jnp.where(above, total, jnp.where(on, diagonal, 0.0))
    added = (sum0[...] + sum1[...]) + (sum2[...] + sum3[...])
    sums[...] = added
    ends = (
        jnp.max(jnp.where(above, jnp.abs(total), 0.0)),
        jnp.max(jnp.where(on, diagonal, -jnp.inf)),
        -jnp.min(jnp.where(on, diagonal, jnp.inf)),
        jnp.max(added),
        -jnp.min(added),
    )
    lane = lax.broadcasted_iota(jnp.int32, levels.shape, 2)
    value = jnp.full(levels.shape, ends[0], jnp.float32)
    for k in range(1, 5):
        value = jnp.where(lane == k, ends[k], value)
    levels[...] = value


def final_kernel(levels, upper, narrow, factor, sums, right, token0, token1, token2, token3, new_factor, new_right):
    first = lax.axis_index(GROUP) * ROWS
    tokens = (token0[...] + token1[...]) + (token2[...] + token3[...])
    weight = (4 * token0[...] / tokens)[:, 0:1]
    squared = weight * weight
    scale = squared / FF2
    peak = jnp.max(levels[...], axis=0)
    off, most, least, sum_most, sum_least = (peak[0:1, k : k + 1] for k in range(5))
    row_peak = jnp.maximum(scale * off, jnp.maximum(jnp.abs(scale * most - 1.0), jnp.abs(-scale * least - 1.0)))
    column_most = jnp.abs(squared * sum_most / DIM - 1.0)
    column_peak = jnp.maximum(column_most, jnp.abs(-squared * sum_least / DIM - 1.0))
    row = lax.broadcasted_iota(jnp.int32, (ROWS, BLOCK), 0) + first
    col = lax.broadcasted_iota(jnp.int32, (ROWS, BLOCK), 1)
    upper_part = upper[...] * scale - jnp.where(row == col, 1.0, 0.0)
    steps = (upper_part / (row_peak + epsilon)).astype(jnp.bfloat16)
    moved = jnp.dot(steps, narrow[...], preferred_element_type=jnp.float32)
    new_factor[0] = factor[0] - step_rate * moved
    term = squared * sums[...] / DIM - 1.0
    new_right[...] = right[...] - step_rate * term / (column_peak + epsilon) * right[...]


def shape(dims, dtype=jnp.float32):
    return jax.ShapeDtypeStruct(dims, dtype)


def call(kernel, ins, outs, flops, scratch=(), room=16):
    return pl.pallas_call(
        kernel,
        out_shape=outs,
        grid=(1,),
        in_specs=ins,
        out_specs=[VMEM] * len(outs),
        scratch_shapes=list(scratch),
        compiler_params=pltpu.CompilerParams(vmem_limit_bytes=room * 1024 * 1024),
        cost_estimate=pl.CostEstimate(flops=flops, bytes_accessed=2097152, transcendentals=0),
    )


def exchange(value, axes):
    return lax.all_to_all(value, axes, 0, 0, tiled=True)


def across(value, turn, axis="zh"):
    return lax.ppermute(value, axis, [(k, k ^ turn) for k in range(4)])


def to_peer(value, dz, dx, dc):
    pairs = []
    for device in range(16):
        plane, x, c = device // 8, device // 2 % 4, device % 2
        pairs.append((device, (plane + dz) % 2 * 8 + (x + dx) % 4 * 2 + (c + dc) % 2))
    return lax.ppermute(value, GROUP, pairs)


def pack(gradient, factor, counts):
    half = jnp.bfloat16
    outs = [shape((ROWS, MESSAGE), half)] * PEERS
    return pl.pallas_call(
        pack_kernel,
        out_shape=outs + [shape((1, 128))],
        in_specs=[HBM, HBM, SMEM],
        out_specs=[VMEM] * (PEERS + 1),
        scratch_shapes=[
            pltpu.VMEM((2, 4, ROWS, HALF), half),
            pltpu.VMEM((1, ROWS, BLOCK), jnp.float32),
            pltpu.SemaphoreType.DMA((9,)),
        ],
        compiler_params=pltpu.CompilerParams(vmem_limit_bytes=51 * 1024 * 1024),
        cost_estimate=pl.CostEstimate(flops=2000000, bytes_accessed=4194304, transcendentals=0),
        name="pack",
    )(gradient, factor, counts)


def inner(gradient, factor, right_diag, counts):
    half = jnp.bfloat16
    *leaving, staying, token = pack(gradient, factor, counts)
    crosses = [to_peer(value, *OFFSETS[k]) for k, value in enumerate(leaving)]
    rights = [right_diag] + [across(right_diag, d) for d in (1, 2, 3)]
    tokens = [token] + [across(token, d, "expert") for d in (1, 2, 3)]
    part, *sums, narrow = call(
        gram_kernel,
        [VMEM] * (PEERS + 4),
        [shape((BLOCK, BLOCK), half)] + [shape((1, OWN))] * 4 + [shape((BLOCK, BLOCK), half)],
        1600000000,
        [pltpu.VMEM((BLOCK, MESSAGE), half), pltpu.VMEM((BLOCK, WIDE), half)],
    )(*rights, staying, *crosses)
    parts = exchange(part.reshape(16, ROWS, BLOCK), GROUP)
    sums = [sums[0]] + [across(sums[d], d) for d in (1, 2, 3)]
    upper, term, levels = call(
        peaks_kernel, [VMEM] * 5, [shape((ROWS, BLOCK)), shape((1, OWN)), shape((64, 1, 128))], 2000000
    )(parts, *sums)
    levels = exchange(levels, SHARD)
    new_factor, new_right = call(
        final_kernel, [VMEM] * 10, [shape((1, ROWS, BLOCK)), shape((1, OWN))], 17000000
    )(levels, upper, narrow, factor, term, right_diag, *tokens)
    return new_factor, new_right


def solution(mesh):
    torus = Mesh(
        mesh.devices.reshape(mesh.shape["expert"], 4, 2, 4, 2),
        ("expert", "zh", "zl", "x", "c"),
    )
    return jax.shard_map(
        inner,
        mesh=torus,
        in_specs=(
            P("expert", SHARD, None),
            P("expert", SHARD, None),
            P("expert", SHARD),
            P("expert"),
        ),
        out_specs=(P("expert", SHARD, None), P("expert", SHARD)),
        check_vma=False,
    )
```

```python
import jax
import jax.numpy as jnp
from jax import lax
from jax.experimental import pallas as pl
from jax.experimental.pallas import tpu as pltpu
from jax.sharding import Mesh
from jax.sharding import PartitionSpec as P


SHARD = ("zh", "zl", "x", "c")
GROUP = ("zl", "x", "c")
FF2 = 28672
DIM = 2048
BLOCK = 512
ROWS = 32
OWN = 448
PAIR = 896
SPAN = 16 * OWN
HALF = 8 * OWN
OFFSETS = (
    (1, 0, 0), (0, 2, 0), (1, 0, 1), (0, 3, 0), (1, 1, 0), (0, 2, 1), (1, 3, 0), (0, 3, 1),
    (1, 1, 1), (0, 1, 0), (1, 3, 1), (0, 1, 1), (1, 2, 0), (1, 2, 1), (0, 0, 1), (0, 0, 0),
)
PEERS = len(OFFSETS)
WIDE = 1792
MESSAGE = BLOCK + WIDE

step_rate = 0.5
epsilon = 1e-06


VMEM = pl.BlockSpec(memory_space=pltpu.VMEM)
HBM = pl.BlockSpec(memory_space=pltpu.HBM)
SMEM = pl.BlockSpec(memory_space=pltpu.SMEM)


def pack_kernel(gradient, factor, counts, *refs):
    outs, notes, (near, rows, sems) = refs[:PEERS], refs[PEERS], refs[PEERS + 1 :]
    block, plane = lax.axis_index("zh"), lax.axis_index("zl")
    x, c = lax.axis_index("x"), lax.axis_index("c")
    fetches = [pltpu.make_async_copy(factor, rows, sems.at[8])]
    for dz in range(2):
        for d in range(4):
            begin = pl.multiple_of((block ^ d) * SPAN + lax.rem(plane + dz, 2) * HALF, 128)
            source = gradient.at[0, :, pl.ds(begin, HALF)]
            fetches.append(pltpu.make_async_copy(source, near.at[dz, d], sems.at[4 * dz + d]))
    for fetch in fetches:
        fetch.start()
    notes[...] = jnp.full(notes.shape, counts[0].astype(jnp.float32), jnp.float32)
    fetches[0].wait()
    narrow = rows[0].astype(jnp.bfloat16)
    for out in outs:
        out[:, :BLOCK] = narrow
    for dz in range(2):
        for fetch in fetches[1 + 4 * dz : 5 + 4 * dz]:
            fetch.wait()
        for dx in range(4):
            begin = pl.multiple_of(lax.rem(x + dx, 4) * PAIR, 128)
            same, other = outs[OFFSETS.index((dz, dx, 0))], outs[OFFSETS.index((dz, dx, 1))]
            for q in range(2):
                pairs = [near[dz, 2 * q + k, :, pl.ds(begin, PAIR)] for k in range(2)]
                even = jnp.concatenate([pair[:, :OWN] for pair in pairs], axis=1)
                odd = jnp.concatenate([pair[:, OWN:] for pair in pairs], axis=1)
                left = BLOCK + q * PAIR
                same[:, left : left + PAIR] = jnp.where(c == 0, even, odd)
                other[:, left : left + PAIR] = jnp.where(c == 0, odd, even)


def gram_kernel(*refs):
    rights, staying = refs[0:4], refs[4]
    crosses, refs = refs[5 : PEERS + 4], refs[5:]
    part, sum0, sum1, sum2, sum3, narrow, got, image = refs[PEERS - 1 :]
    plane, x, c = lax.axis_index("zl"), lax.axis_index("x"), lax.axis_index("c")
    own = pl.multiple_of((plane * 8 + x * 2 + c) * ROWS, ROWS)
    got[pl.ds(own, ROWS), :] = staying[...]
    for k, (dz, dx, dc) in enumerate(OFFSETS[:-1]):
        source = lax.rem(plane + dz, 2) * 8 + lax.rem(x + (4 - dx), 4) * 2 + lax.rem(c + dc, 2)
        got[pl.ds(pl.multiple_of(source * ROWS, ROWS), ROWS), :] = crosses[k][...]
    narrow[...] = got[:, :BLOCK]
    right = jnp.concatenate([one[...] for one in rights], axis=1)
    upper_left = got[0:256, 0:512]
    lower_right = got[256:512, 256:512]
    totals = []
    for k in range(7):
        at = BLOCK + k * 256
        scale = right[:, k * 256 : (k + 1) * 256]
        high = jnp.dot(upper_left, got[:, at : at + 256], preferred_element_type=jnp.float32)
        low = jnp.dot(lower_right, got[256:512, at : at + 256], preferred_element_type=jnp.float32)
        high = (high * scale).astype(jnp.bfloat16)
        low = (low * scale).astype(jnp.bfloat16)
        image[0:256, k * 256 : (k + 1) * 256] = high
        image[256:512, k * 256 : (k + 1) * 256] = low
        total = jnp.sum(jnp.square(high.astype(jnp.float32)), axis=0, keepdims=True)
        total = total + jnp.sum(jnp.square(low.astype(jnp.float32)), axis=0, keepdims=True)
        totals.append(total)
    total = jnp.concatenate(totals, axis=1)
    for d, out in enumerate((sum0, sum1, sum2, sum3)):
        out[...] = total[:, d * OWN : (d + 1) * OWN]
    last = (((1,), (1,)), ((), ()))
    high = lax.dot_general(image[0:256, :], image[...], last, preferred_element_type=jnp.float32)
    low = lax.dot_general(image[256:512, :], image[256:512, :], last, preferred_element_type=jnp.float32)
    row = lax.broadcasted_iota(jnp.int32, (256, 256), 0)
    col = lax.broadcasted_iota(jnp.int32, (256, 256), 1)
    on = row == col
    slot = jnp.logical_and(row % ROWS == ROWS - 1, col == row - (ROWS - 1))
    corners = (high[:, 0:256], low)
    least = [jnp.min(jnp.where(on, corner, jnp.inf)) for corner in corners]
    share = jnp.full((8, 128), jnp.minimum(*least), jnp.float32).astype(part.dtype).astype(jnp.float32)[0:1, 0:1]
    shared = [jnp.where(slot, share, jnp.where(on, corner - share, corner)).astype(part.dtype) for corner in corners]
    part[0:256, 0:256], part[256:512, 256:512] = shared
    part[0:256, 256:512] = high[:, 256:512].astype(part.dtype)
    part[256:512, 0:256] = jnp.zeros((256, 256), part.dtype)


def peaks_kernel(parts, sum0, sum1, sum2, sum3, upper, sums, levels):
    first = lax.axis_index(GROUP) * ROWS
    total = parts[0].astype(jnp.float32)
    for k in range(1, 16):
        total = total + parts[k].astype(jnp.float32)
    place = lax.broadcasted_iota(jnp.int32, (ROWS, BLOCK), 0)
    row = place + first
    col = lax.broadcasted_iota(jnp.int32, (ROWS, BLOCK), 1)
    share = jnp.sum(jnp.where(jnp.logical_and(place == ROWS - 1, col == first), total, 0.0))
    diagonal = total + share
    above, on = col > row, col == row
    upper[...] = jnp.where(above, total, jnp.where(on, diagonal, 0.0))
    added = (sum0[...] + sum1[...]) + (sum2[...] + sum3[...])
    sums[...] = added
    ends = (
        jnp.max(jnp.where(above, jnp.abs(total), 0.0)),
        jnp.max(jnp.where(on, diagonal, -jnp.inf)),
        -jnp.min(jnp.where(on, diagonal, jnp.inf)),
        jnp.max(added),
        -jnp.min(added),
    )
    lane = lax.broadcasted_iota(jnp.int32, levels.shape, 2)
    value = jnp.full(levels.shape, ends[0], jnp.float32)
    for k in range(1, 5):
        value = jnp.where(lane == k, ends[k], value)
    levels[...] = value


def final_kernel(levels, upper, narrow, factor, sums, right, token0, token1, token2, token3, new_factor, new_right):
    first = lax.axis_index(GROUP) * ROWS
    tokens = (token0[...] + token1[...]) + (token2[...] + token3[...])
    weight = (4 * token0[...] / tokens)[:, 0:1]
    squared = weight * weight
    scale = squared / FF2
    peak = jnp.max(levels[...], axis=0)
    off, most, least, sum_most, sum_least = (peak[0:1, k : k + 1] for k in range(5))
    row_peak = jnp.maximum(scale * off, jnp.maximum(jnp.abs(scale * most - 1.0), jnp.abs(-scale * least - 1.0)))
    column_most = jnp.abs(squared * sum_most / DIM - 1.0)
    column_peak = jnp.maximum(column_most, jnp.abs(-squared * sum_least / DIM - 1.0))
    row = lax.broadcasted_iota(jnp.int32, (ROWS, BLOCK), 0) + first
    col = lax.broadcasted_iota(jnp.int32, (ROWS, BLOCK), 1)
    upper_part = upper[...] * scale - jnp.where(row == col, 1.0, 0.0)
    steps = (upper_part / (row_peak + epsilon)).astype(jnp.bfloat16)
    moved = jnp.dot(steps, narrow[...], preferred_element_type=jnp.float32)
    new_factor[0] = factor[0] - step_rate * moved
    term = squared * sums[...] / DIM - 1.0
    new_right[...] = right[...] - step_rate * term / (column_peak + epsilon) * right[...]


def shape(dims, dtype=jnp.float32):
    return jax.ShapeDtypeStruct(dims, dtype)


def call(kernel, ins, outs, flops, scratch=(), room=16):
    return pl.pallas_call(
        kernel,
        out_shape=outs,
        grid=(1,),
        in_specs=ins,
        out_specs=[VMEM] * len(outs),
        scratch_shapes=list(scratch),
        compiler_params=pltpu.CompilerParams(vmem_limit_bytes=room * 1024 * 1024),
        cost_estimate=pl.CostEstimate(flops=flops, bytes_accessed=2097152, transcendentals=0),
    )


def exchange(value, axes):
    return lax.all_to_all(value, axes, 0, 0, tiled=True)


def across(value, turn, axis="zh"):
    return lax.ppermute(value, axis, [(k, k ^ turn) for k in range(4)])


def to_peer(value, dz, dx, dc):
    pairs = []
    for device in range(16):
        plane, x, c = device // 8, device // 2 % 4, device % 2
        pairs.append((device, (plane + dz) % 2 * 8 + (x + dx) % 4 * 2 + (c + dc) % 2))
    return lax.ppermute(value, GROUP, pairs)


def pack(gradient, factor, counts):
    half = jnp.bfloat16
    outs = [shape((ROWS, MESSAGE), half)] * PEERS
    return pl.pallas_call(
        pack_kernel,
        out_shape=outs + [shape((1, 128))],
        in_specs=[HBM, HBM, SMEM],
        out_specs=[VMEM] * (PEERS + 1),
        scratch_shapes=[
            pltpu.VMEM((2, 4, ROWS, HALF), half),
            pltpu.VMEM((1, ROWS, BLOCK), jnp.float32),
            pltpu.SemaphoreType.DMA((9,)),
        ],
        compiler_params=pltpu.CompilerParams(vmem_limit_bytes=51 * 1024 * 1024),
        cost_estimate=pl.CostEstimate(flops=2000000, bytes_accessed=4194304, transcendentals=0),
        name="pack",
    )(gradient, factor, counts)


def inner(gradient, factor, right_diag, counts):
    half = jnp.bfloat16
    *leaving, staying, token = pack(gradient, factor, counts)
    crosses = [to_peer(value, *OFFSETS[k]) for k, value in enumerate(leaving)]
    rights = [right_diag] + [across(right_diag, d) for d in (1, 2, 3)]
    tokens = [token] + [across(token, d, "expert") for d in (1, 2, 3)]
    part, *sums, narrow = call(
        gram_kernel,
        [VMEM] * (PEERS + 4),
        [shape((BLOCK, BLOCK), half)] + [shape((1, OWN))] * 4 + [shape((BLOCK, BLOCK), half)],
        1600000000,
        [pltpu.VMEM((BLOCK, MESSAGE), half), pltpu.VMEM((BLOCK, WIDE), half)],
    )(*rights, staying, *crosses)
    parts = exchange(part.reshape(16, ROWS, BLOCK), GROUP)
    sums = [sums[0]] + [across(sums[d], d) for d in (1, 2, 3)]
    upper, term, levels = call(
        peaks_kernel,
        [VMEM] * 5,
        [shape((ROWS, BLOCK)), shape((1, OWN)), shape((64, 1, 128))],
        2000000,
    )(parts, *sums)
    levels = exchange(levels, SHARD)
    new_factor, new_right = call(
        final_kernel, [VMEM] * 10, [shape((1, ROWS, BLOCK)), shape((1, OWN))], 17000000
    )(levels, upper, narrow, factor, term, right_diag, *tokens)
    return new_factor, new_right


def solution(mesh):
    torus = Mesh(
        mesh.devices.reshape(mesh.shape["expert"], 4, 2, 4, 2),
        ("expert", "zh", "zl", "x", "c"),
    )
    return jax.shard_map(
        inner,
        mesh=torus,
        in_specs=(
            P("expert", SHARD, None),
            P("expert", SHARD, None),
            P("expert", SHARD),
            P("expert"),
        ),
        out_specs=(P("expert", SHARD, None), P("expert", SHARD)),
        check_vma=False,
    )
```
